256 devices in a mesh: row: 32 (over z, y), col: 8 (over x, core).
Axes of the slice: x: 4, y: 4, z: 8, core: 2. Of those that a mesh axis runs over, the one named last changes fastest.
Arguments:
- coeffs: bfloat16 [32768, 1024], P(('row', 'col')), may hold values from -0.125 to 0.125
- h_blocks: bfloat16 [32, 8, 32, 4, 128, 128], P('row', 'col'), may hold values from -18 to 18
- block_codes: int32 [32, 8, 32, 4], P('row', 'col'), may hold values from 0 to 8, as said below
Outputs:
- gram: float32 [1024, 1024], P('row', 'col')
The draws below stay inside these ranges and needn't reach their ends.
Inputs may be any that keep to these rules, and one draw needn't show every extreme that they name: The value 8 * 1 marks an empty slot; the other values within one sub-panel block_codes[r, c, p, :] are distinct. Every tile [r, c] has a sub-panel with no empty slot.
All inputs are finite; a program needn't handle non-finite values.
Results may differ from the reference program's by a relative error of at most 0.0003.
Values may be sent and summed in bfloat16 or wider, within the bound.
No kernel may reach another device: no remote copies, remote signals or barrier semaphores. Data moves between devices by JAX's collectives and lax.ppermute only.
A program may use at most 128 MiB of HBM per device.

```python
import jax
import jax.numpy as jnp
from jax import lax

BLK = 128
ORBITALS = 1024
CAP = 4
ORDER = 32768
PANEL_BLOCKS = 1
TILE_BROWS = 8
N_ROW = 32
N_COL = 8


def draw_block_codes(key, part):
    slot_count = TILE_BROWS * PANEL_BLOCKS
    panels = N_ROW * N_COL * N_ROW
    key_order, key_count, key_full = jax.random.split(jax.random.fold_in(key, 11), 3)
    scores = jax.random.randint(key_order, (panels, slot_count), 0, 1 << 20) * slot_count + jnp.arange(slot_count, dtype=jnp.int32)[None, :]
    ranked = jnp.argsort(scores, axis=1)[:, :CAP].astype(jnp.int32)
    counts = jax.random.randint(key_count, (N_ROW * N_COL, N_ROW), 2, CAP + 1)
    full_index = jax.random.randint(key_full, (N_ROW * N_COL, 1), 0, N_ROW)
    counts = jnp.where(jnp.arange(N_ROW)[None, :] == full_index, CAP, counts).reshape(panels, 1)
    is_live = jnp.arange(CAP)[None, :] < counts
    codes_all = jnp.where(is_live, ranked, slot_count)
    return codes_all.reshape(N_ROW, N_COL, N_ROW, CAP).astype(jnp.int32)


def strengthened(entries, stream_key, source, target, blocks, factor):
    owner, partner = [(jnp.arange(entries.shape[dim]) // (entries.shape[dim] // blocks)).reshape([-1 if axis == dim else 1 for axis in range(entries.ndim)]) for dim in (source, target)]
    chosen = jax.random.permutation(stream_key, blocks)[partner]
    strong = (owner == chosen) | (owner == (partner + blocks // 2) % blocks)
    return jnp.where(strong, factor * entries, entries)


def block_scale(rng, extent, pieces, least, largest):
    gain, own = 1.0, jax.random.fold_in(rng, 6)
    for dim, parts in pieces:
        heights = jnp.exp(jax.random.uniform(jax.random.fold_in(own, dim), (parts,), jnp.float32, least / len(pieces), largest / len(pieces)))
        gain = gain * jnp.repeat(heights, extent[dim] // parts).reshape([-1 if axis == dim else 1 for axis in range(len(extent))])
    return gain


def normal_values(stream_key, extent, scale, limit, shards=(), held_as=jnp.bfloat16):
    array = jax.random.normal(stream_key, extent, jnp.float32) * scale
    if len(shards) > 0:
        array = block_scale(stream_key, extent, shards, -0.22, 0.18) * array
    return jnp.clip(array, min=-limit, max=limit).astype(held_as)


def bell_draw_with(own_key, shape, width, most, cuts, heavy, kind=jnp.bfloat16):
    drawn = width * jax.random.normal(own_key, shape, jnp.float32)
    if cuts:
        drawn = drawn * block_scale(own_key, shape, cuts, -0.22, 0.18)
    return jnp.clip(strengthened(drawn, jax.random.fold_in(own_key, 3), *heavy), -most, most).astype(kind)


def setup_inputs(seed: int = 0) -> dict:
    streams_of = jax.random.split(jax.random.key(seed), 4)
    return {
        "coeffs": bell_draw_with(streams_of[0], (ORDER, ORBITALS), ORDER ** -0.5, 0.125, ((0, 256),), (0, 1, 256, 6.0)),
        "h_blocks": normal_values(streams_of[1], (N_ROW, N_COL, N_ROW, CAP, BLK, BLK), 3.0, 18.0, ((0, 32), (1, 8))),
        "block_codes": draw_block_codes(jax.random.fold_in(streams_of[3], 71), 0),
    }


def tile_product(coeffs, h_blocks, block_codes, row_index):
    orbital_width = coeffs.shape[1]
    empty_code = TILE_BROWS * PANEL_BLOCKS
    panel_data = coeffs.reshape(N_ROW, N_COL, PANEL_BLOCKS, BLK, orbital_width).transpose(1, 0, 2, 3, 4)
    row_blocks = lax.dynamic_index_in_dim(h_blocks, row_index, 0, keepdims=False)
    row_codes = lax.dynamic_index_in_dim(block_codes, row_index, 0, keepdims=False)

    def add_tile(running, inputs):
        blocks, codes, panel = inputs
        is_live = (codes < empty_code).astype(jnp.float32)
        block_row = jnp.minimum(codes // PANEL_BLOCKS, TILE_BROWS - 1).astype(jnp.int32)
        within = (codes % PANEL_BLOCKS).astype(jnp.int32)
        selector = (within[:, :, None] == jnp.arange(PANEL_BLOCKS, dtype=jnp.int32)[None, None, :]).astype(jnp.float32)
        chosen = jnp.einsum("psq,pqjk->psjk", selector, panel.astype(jnp.float32))
        product = jnp.einsum("psij,psjk->psik", blocks.astype(jnp.float32), chosen) * is_live[:, :, None, None]
        running = running.at[block_row.reshape(-1)].add(product.reshape(-1, BLK, orbital_width))
        return running, None

    zero_rows = jnp.zeros((TILE_BROWS, BLK, orbital_width), jnp.float32)
    result, unused = lax.scan(add_tile, zero_rows, (row_blocks, row_codes, panel_data))
    return result.reshape(TILE_BROWS * BLK, orbital_width)


def reference(coeffs, h_blocks, block_codes):
    orbital_width = coeffs.shape[1]
    group_rows = TILE_BROWS * BLK

    def add_group(gram, row_index):
        applied = tile_product(coeffs, h_blocks, block_codes, row_index)
        left_rows = lax.dynamic_slice_in_dim(coeffs, row_index * group_rows, group_rows, 0).astype(jnp.float32)
        gram = gram + jnp.dot(left_rows.T, applied, precision=lax.Precision.HIGHEST)
        return gram, None

    start_gram = jnp.zeros((orbital_width, orbital_width), jnp.float32)
    gram, unused = lax.scan(add_group, start_gram, jnp.arange(N_ROW, dtype=jnp.int32))
    return gram
```

```python
import functools

import jax
import jax.numpy as jnp
from jax import lax
from jax.experimental import pallas as pl
from jax.experimental.pallas import tpu as pltpu
from jax.sharding import PartitionSpec as P

BLK = 128
CAP = 4
NX, NY, NZ = 4, 4, 8
DZ = (0, -1, 1, -2, 2, -3, 3, 4)
DY = (0, -1, 1, 2)

VMEM = pl.BlockSpec(memory_space=pltpu.VMEM)
SMEM = pl.BlockSpec(memory_space=pltpu.SMEM)


def move_row(v, dz, dy):
    pairs = [
        (z * NY + y, (z + dz) % NZ * NY + (y + dy) % NY) for z in range(NZ) for y in range(NY)
    ]
    return lax.ppermute(v, "row", pairs)


def move_col(v, dx, dc):
    pairs = [
        (x * 2 + c, (x + dx) % NX * 2 + (c + dc) % 2) for x in range(NX) for c in range(2)
    ]
    return lax.ppermute(v, "col", pairs)


def dense_kernel(order_ref, code_ref, h_ref, out_ref):
    j = pl.program_id(0)
    panel = order_ref[j]
    out_ref[...] = jnp.zeros_like(out_ref)
    for s in range(CAP):
        code = code_ref[panel, s]

        @pl.when(code < 8)
        def _():
            out_ref[0, pl.ds(pl.multiple_of(code * BLK, BLK), BLK), :] = h_ref[0, s]


def dense_panels(blocks, codes, order, rows):
    panels = blocks.shape[0]
    return pl.pallas_call(
        dense_kernel,
        grid_spec=pltpu.PrefetchScalarGridSpec(
            num_scalar_prefetch=2,
            grid=(panels,),
            in_specs=[pl.BlockSpec((1, CAP, BLK, BLK), lambda j, o, c: (o[j], 0, 0, 0))],
            out_specs=pl.BlockSpec((1, rows, BLK), lambda j, o, c: (j, 0, 0)),
        ),
        out_shape=jax.ShapeDtypeStruct((panels, rows, BLK), jnp.bfloat16),
        cost_estimate=pl.CostEstimate(flops=0, bytes_accessed=16 << 20, transcendentals=0),
    )(order, codes, blocks)


def early_kernel(slots_a, slots_b, h_ref, *refs):
    a_refs, b_refs = refs[: len(slots_a)], refs[len(slots_a) : -2]
    out_a, out_b = refs[-2:]
    tile = 256

    @pl.loop(0, out_a.shape[0] // tile)
    def _(i):
        rows = pl.ds(pl.multiple_of(i * tile, tile), tile)
        for slots, c_refs, out in ((slots_a, a_refs, out_a), (slots_b, b_refs, out_b)):
            total = None
            for mine, c_ref in zip(slots, c_refs):
                left = jnp.concatenate([h_ref[s, rows, :] for s in mine], axis=1)
                term = jnp.dot(left, c_ref[...], preferred_element_type=jnp.float32)
                total = term if total is None else total + term
            out[rows, :] = total


def late_kernel(slots_a, slots_b, place_ref, h_ref, acc_a, acc_b, *refs):
    a_refs, b_refs = refs[: len(slots_a)], refs[len(slots_a) : -1]
    out_ref = refs[-1]
    tile = 256
    x, core = place_ref[0], place_ref[1]

    @pl.loop(0, acc_a.shape[0] // tile)
    def _(i):
        rows = pl.ds(pl.multiple_of(i * tile, tile), tile)
        for parity, (slots, c_refs, acc) in enumerate(
            ((slots_a, a_refs, acc_a), (slots_b, b_refs, acc_b))
        ):
            total = acc[rows, :]
            for mine, c_ref in zip(slots, c_refs):
                left = jnp.concatenate([h_ref[s, rows, :] for s in mine], axis=1)
                total = total + jnp.dot(left, c_ref[...], preferred_element_type=jnp.float32)
            for to in range(NX):
                out_ref[(parity + core) % 2, (to - x + NX) % NX, rows, :] = total[
                    :, to * BLK : (to + 1) * BLK
                ]


def gram_kernel(left_ref, own_ref, more_ref, out_ref):
    applied = own_ref[...] + more_ref[...]
    high = applied.astype(jnp.bfloat16)
    low = (applied - high.astype(jnp.float32)).astype(jnp.bfloat16)
    both = jnp.concatenate([high, low], axis=1)
    for z in range(NZ):
        full = lax.dot_general(
            left_ref[:, z * BLK : (z + 1) * BLK],
            both,
            (((0,), (0,)), ((), ())),
            preferred_element_type=jnp.float32,
        )
        part = full[:, :BLK] + full[:, BLK:]
        for y in range(NY):
            out_ref[y, z] = part[y * 32 : (y + 1) * 32]


def shards(coeffs, h_blocks, block_codes):
    panels = NY * NZ
    rows = BLK * 8
    row = lax.axis_index("row")
    col = lax.axis_index("col")
    z, y, x, core = row // NY, row % NY, col // 2, col % 2
    blocks = h_blocks.reshape(panels, CAP, BLK, BLK)
    codes = block_codes.reshape(panels, CAP)
    dz = jnp.array(DZ, jnp.int32)[:, None]
    dy = jnp.array(DY, jnp.int32)[None, :]
    order = ((z + dz + NZ) % NZ * NY + (y + dy + NY) % NY).reshape(-1)
    dense = dense_panels(blocks, codes, order, rows)

    by_chunk = coeffs.reshape(BLK, NX, 2, BLK)
    even = by_chunk[:, :, 0].reshape(BLK, NX * BLK)
    odd = by_chunk[:, :, 1].reshape(BLK, NX * BLK)

    zb = {0: odd, -1: move_row(odd, 1, 0), 1: move_row(odd, -1, 0)}
    ya = {0: even, -1: move_row(even, 0, 1), 1: move_row(even, 0, -1)}
    left = lax.all_to_all(jnp.broadcast_to(coeffs[None], (8, *coeffs.shape)), "col", 0, 0, tiled=True)
    left = left.reshape(rows, coeffs.shape[1])
    zb[-2], zb[2] = move_row(zb[-1], 1, 0), move_row(zb[1], -1, 0)
    ya[2] = move_row(ya[1], 0, -1)
    zb[-3], zb[3] = move_row(zb[-2], 1, 0), move_row(zb[2], -1, 0)
    zb[4] = move_row(zb[3], -1, 0)
    za = {0: jnp.concatenate([ya[k] for k in DY], axis=0)}
    yb = {0: jnp.concatenate([zb[k] for k in DZ], axis=0)}
    for k in (1, 2, 3):
        za[-k], za[k] = move_row(za[1 - k], 1, 0), move_row(za[k - 1], -1, 0)
    za[4] = move_row(za[-3], 1, 0)
    yb[-1], yb[1] = move_row(yb[0], 0, 1), move_row(yb[0], 0, -1)
    half = rows // 2
    across = [move_row(yb[-1][:half], 0, 1), move_row(yb[1][half:], 0, -1)]

    slots_a = {k: [DZ.index(k) * NY + i for i in range(NY)] for k in DZ}
    slots_b = {k: [i * NY + DY.index(k) for i in range(NZ)] for k in DY}
    early_a, early_b = (0, -1, 1, -2, 2), (0, -1, 1)
    width = NX * BLK
    acc_a, acc_b = pl.pallas_call(
        functools.partial(early_kernel, [slots_a[k] for k in early_a], [slots_b[k] for k in early_b]),
        in_specs=[VMEM] * 9,
        out_specs=[VMEM] * 2,
        out_shape=[jax.ShapeDtypeStruct((rows, width), jnp.float32)] * 2,
        cost_estimate=pl.CostEstimate(flops=6 << 30, bytes_accessed=16 << 20, transcendentals=0),
    )(dense, *(za[k] for k in early_a), *(yb[k] for k in early_b))
    late_a = (-3, 3, 4)
    parts = pl.pallas_call(
        functools.partial(
            late_kernel,
            [slots_a[k] for k in late_a],
            [slots_b[2][: NZ // 2], slots_b[2][NZ // 2 :]],
        ),
        in_specs=[SMEM] + [VMEM] * 8,
        out_specs=VMEM,
        out_shape=jax.ShapeDtypeStruct((2, NX, rows, BLK), jnp.float32),
        cost_estimate=pl.CostEstimate(flops=3 << 30, bytes_accessed=16 << 20, transcendentals=0),
    )(jnp.stack([x, core]).astype(jnp.int32), dense, acc_a, acc_b, *(za[k] for k in late_a), *across)

    here = parts[0] + move_col(parts[1], 0, 1)
    from_left = move_col(here[2, :half], 1, 0)
    from_right = move_col(here[2, half:], -1, 0)
    to_right = here[1] + jnp.pad(from_left, ((0, half), (0, 0)))
    to_left = here[3] + jnp.pad(from_right, ((half, 0), (0, 0)))
    more = move_col(to_right, 1, 0) + move_col(to_left, -1, 0)
    gram = pl.pallas_call(
        gram_kernel,
        in_specs=[VMEM] * 3,
        out_specs=VMEM,
        out_shape=jax.ShapeDtypeStruct((NY, NZ, 32, BLK), jnp.float32),
        cost_estimate=pl.CostEstimate(flops=1 << 29, bytes_accessed=4 << 20, transcendentals=0),
    )(left, here[0], more)
    y_groups = [[i * NY + j for j in range(NY)] for i in range(NZ)]
    z_groups = [[i * NY + j for i in range(NZ)] for j in range(NY)]
    gram = jnp.sum(lax.all_to_all(gram, "row", 0, 0, axis_index_groups=y_groups, tiled=True), axis=0)
    gram = jnp.sum(lax.all_to_all(gram, "row", 0, 0, axis_index_groups=z_groups, tiled=True), axis=0)
    return gram


def solution(mesh):
    return jax.shard_map(
        shards,
        mesh=mesh,
        in_specs=(
            P(("row", "col"), None),
            P("row", "col", None, None, None, None),
            P("row", "col", None, None),
        ),
        out_specs=P("row", "col"),
        check_vma=False,
    )
```
